1024 devices in a mesh: rows: 32 (over y_hi, x), cols: 4 (over y_lo, core), reps: 8 (over z).
Axes of the slice: x: 8, y: 8 (y_hi: 4, y_lo: 2; y = y_hi * 2 + y_lo), z: 8, core: 2. Of those that a mesh axis runs over, the one named last changes fastest.
Arguments:
- features: bfloat16 [32768, 512], P('rows', 'cols'), may hold values from -6 to 6
- tiles: bfloat16 [65536, 128, 128], P(('rows', 'reps')), may hold values from -0.1875 to 0.1875
- tile_cols: int32 [256, 256], P(('rows', 'reps')), may hold values from 0 to 255, as said below
- tile_ptr: int32 [256, 33], P(('rows', 'reps')), may hold values from 0 to 256, as said below
Outputs:
- aggregated: bfloat16 [32768, 512], P(('rows', 'reps'), 'cols')
The draws below stay inside these ranges and needn't reach their ends.
Inputs may be any that keep to these rules, and one draw needn't show every extreme that they name: `tile_cols`: slot j of row g = b * 8 + q with key k (see steps) lies in section s = k // 8; its column tile is c * 8 + e with column block c = (b + q * 4 + s) mod 32 and 0 <= e < 8. Live slots name distinct tiles and are in order of key. Slots that are not live hold 0 and arbitrary tile values. `tile_ptr`: each row starts at 0 and never falls; its last entry, the live count, is at least 1 and equals 256 on some row of every draw; counts are skewed, most rows holding a quarter of 256 or less.
All inputs are finite; a program needn't handle non-finite values.
Results may differ from the reference program's by a relative error of at most 0.001.
Values may be sent and summed in bfloat16 or wider, within the bound.
No kernel may reach another device: no remote copies, remote signals or barrier semaphores. Data moves between devices by JAX's collectives and lax.ppermute only.
A program may use at most 64 MiB of HBM per device.

```python
import jax
import jax.numpy as jnp
from jax import lax

TILE = 128
FEAT = 512
TB = 8
SECTIONS = 4
SLOTS = 256
NODES = 32768
N_ROWS = 32
N_REPS = 8


def tile_layout(key):
    base = jax.random.fold_in(key, 11)
    key_a, key_b, key_c, key_d = jax.random.split(base, 4)
    num_devices = N_ROWS * N_REPS
    level_a = jax.random.randint(key_a, (num_devices,), 0, 4)
    level_b = jax.random.randint(key_b, (num_devices,), 0, 4)
    levels = jnp.maximum(level_a, level_b).astype(jnp.int32)
    counts = jnp.right_shift(jnp.full((num_devices,), SLOTS, jnp.int32), levels)
    counts = jnp.maximum(counts, 1)
    fullest = jax.random.randint(key_c, (), 0, num_devices)
    device_ids = jnp.arange(num_devices, dtype=jnp.int32)
    counts = jnp.where(device_ids == fullest, SLOTS, counts).astype(jnp.int32)

    def shuffled(sub_key):
        return jax.random.permutation(sub_key, SLOTS)
    orders = jax.vmap(shuffled)(jax.random.split(key_d, num_devices))
    ranks = jnp.argsort(orders, axis=1).astype(jnp.int32)
    chosen = ranks < counts[:, None]
    positions = jnp.argsort(1 - chosen.astype(jnp.int32), axis=1, stable=True).astype(jnp.int32)
    valid = jnp.arange(SLOTS, dtype=jnp.int32)[None, :] < counts[:, None]
    section_of = positions // (TB * TB)
    within = positions % TB
    row_block = device_ids // N_REPS
    replica = device_ids % N_REPS
    col_block = (row_block[:, None] + replica[:, None] * SECTIONS + section_of) % N_ROWS
    col_ids = jnp.where(valid, col_block * TB + within, 0).astype(jnp.int32)
    pos_keys = jnp.arange(SLOTS, dtype=jnp.int32) // TB
    marks = jnp.arange(SECTIONS * TB + 1, dtype=jnp.int32)
    pointers = jnp.sum((chosen[:, None, :] & (pos_keys[None, None, :] < marks[None, :, None])).astype(jnp.int32), axis=2)
    return (col_ids, pointers.astype(jnp.int32))


def draw_tile_cols(key, part):
    return tile_layout(key)[0]


def draw_tile_ptr(key, part):
    return tile_layout(key)[1]


def shard_levels(rng, extent, cuts, least, largest):
    def one(axis_at, shards_of):
        draws = jax.random.uniform(jax.random.fold_in(jax.random.fold_in(rng, 6), axis_at), (shards_of,), jnp.float32, least / len(cuts), largest / len(cuts))
        return jnp.repeat(jnp.exp(draws), extent[axis_at] // shards_of).reshape((-1,) + (1,) * (len(extent) - axis_at - 1))

    loudness = one(*cuts[0])
    for cut in cuts[1:]:
        loudness = loudness * one(*cut)
    return loudness


def scatter_about(own_key, shape, scale, reach, shards=(), kind=jnp.bfloat16):
    values = scale * jax.random.normal(own_key, shape, jnp.float32)
    if shards:
        values = values * shard_levels(own_key, shape, shards, -0.22, 0.18)
    return jnp.clip(values, -reach, reach).astype(kind)


def setup_inputs(seed: int = 0) -> dict:
    keys = jax.random.split(jax.random.key(seed), 5)
    features = scatter_about(keys[0], (NODES, FEAT), 1.0, 6.0, ((0, 32), (1, 4)))
    tiles = scatter_about(keys[1], (N_ROWS * N_REPS * SLOTS, TILE, TILE), (TILE * TB) ** -0.5, 0.1875, ((0, 256),))
    tile_cols = draw_tile_cols(jax.random.fold_in(keys[4], 71), 0)
    tile_ptr = draw_tile_ptr(jax.random.fold_in(keys[4], 71), 0)
    return dict(features=features, tiles=tiles, tile_cols=tile_cols, tile_ptr=tile_ptr)


def slot_rows(pointers, num_slots):
    slot_ids = jnp.arange(num_slots, dtype=jnp.int32)
    slot_keys = jnp.sum((pointers[None, 1:] <= slot_ids[:, None]).astype(jnp.int32), axis=1)
    return (slot_keys % TB).astype(jnp.int32)


def reference(features, tiles, tile_cols, tile_ptr):
    num_slots = tile_cols.shape[1]
    feat_tiles = features.reshape(N_ROWS * TB, TILE, FEAT)
    dev_tiles = tiles.reshape(N_ROWS * N_REPS, num_slots, TILE, TILE)
    row_range = jnp.arange(TB, dtype=jnp.int32)

    def per_row_block(row_block):
        def one_device(replica, totals):
            device_num = (row_block * N_REPS + replica).astype(jnp.int32)
            own_tiles = dev_tiles[device_num]
            col_ids = tile_cols[device_num]
            pointers = tile_ptr[device_num]
            live_count = pointers[-1]
            row_ids = slot_rows(pointers, num_slots)
            num_blocks = (live_count + TB - 1) // TB

            def advance(block_num, inner):
                begin_at = (block_num * TB).astype(jnp.int32)
                tile_block = lax.dynamic_slice_in_dim(own_tiles, begin_at, TB, 0).astype(jnp.float32)
                col_block = lax.dynamic_slice_in_dim(col_ids, begin_at, TB, 0)
                row_block_ids = lax.dynamic_slice_in_dim(row_ids, begin_at, TB, 0)
                slot_ids = begin_at + jnp.arange(TB, dtype=jnp.int32)
                active = slot_ids < live_count
                feat_block = jnp.take(feat_tiles, col_block, axis=0).astype(jnp.float32)
                products = jnp.einsum("bij,bjf->bif", tile_block, feat_block, precision=lax.Precision.HIGHEST)
                row_onehot = ((row_block_ids[:, None] == row_range[None, :]) & active[:, None]).astype(jnp.float32)
                return inner + jnp.einsum("bt,bif->tif", row_onehot, products, precision=lax.Precision.HIGHEST)

            empty = jnp.zeros((TB, TILE, FEAT), jnp.float32)
            return totals + lax.fori_loop(0, num_blocks, advance, empty)

        return lax.fori_loop(0, N_REPS, one_device, jnp.zeros((TB, TILE, FEAT), jnp.float32))

    sums = lax.map(per_row_block, jnp.arange(N_ROWS, dtype=jnp.int32))
    return sums.reshape(NODES, FEAT).astype(jnp.bfloat16)
```

```python
import functools

import jax
import jax.numpy as jnp
from jax import lax
from jax.experimental import pallas as pl
from jax.experimental.pallas import tpu as pltpu
from jax.sharding import PartitionSpec as P

TB = 8
MIDDLE = 1


def moved(block, rows, reps, source):
    route = []
    for row in range(rows):
        for rep in range(reps):
            from_row, from_rep = source(row, rep)
            route.append((from_row % rows * reps + from_rep % reps, row * reps + rep))
    return lax.ppermute(block, ("rows", "reps"), route)


def section_kernel(sections, chained, cols, ptr, tiles, *refs):
    feats = refs[: len(sections)]
    rest = refs[len(sections) :]
    if chained:
        start, total, dense, sem = rest
    else:
        total, dense, sem = rest
    size = tiles.shape[1]
    for at in range(len(sections)):
        dense[at] = jnp.zeros(dense.shape[1:], dense.dtype)

    def tile_copy(slot, at, row, entry):
        where = dense.at[
            at, pl.ds(row * size, size), pl.ds(pl.multiple_of(entry * size, size), size)
        ]
        return pltpu.make_async_copy(tiles.at[slot], where, sem)

    for at, section in enumerate(sections):
        for row in range(TB):
            key = section * TB + row

            def send(slot, carry, at=at, row=row):
                tile_copy(slot, at, row, lax.rem(cols[0, slot], TB)).start()
                return carry

            lax.fori_loop(ptr[0, key], ptr[0, key + 1], send, 0)
    for at, section in enumerate(sections):

        def arrive(slot, carry):
            tile_copy(0, 0, 0, 0).wait()
            return carry

        lax.fori_loop(ptr[0, section * TB], ptr[0, section * TB + TB], arrive, 0)
    value = start[...] if chained else None
    for at in range(len(sections)):
        part = jnp.dot(dense[at], feats[at][...], preferred_element_type=jnp.float32)
        value = part if value is None else value + part
    total[...] = value


def sections_sum(sections, cols, ptr, tiles, feats, start=None):
    size = tiles.shape[1]
    width = feats[0].shape[1]
    chained = start is not None
    whole = pl.BlockSpec(memory_space=pltpu.VMEM)
    scalars = pl.BlockSpec(memory_space=pltpu.SMEM)
    operands = [cols, ptr, tiles, *feats] + ([start] if chained else [])
    return pl.pallas_call(
        functools.partial(section_kernel, sections, chained),
        out_shape=jax.ShapeDtypeStruct((TB * size, width), jnp.float32),
        in_specs=[scalars, scalars, pl.BlockSpec(memory_space=pl.ANY)]
        + [whole] * (len(operands) - 3),
        out_specs=whole,
        scratch_shapes=[
            pltpu.VMEM((len(sections), TB * size, TB * size), tiles.dtype),
            pltpu.SemaphoreType.DMA,
        ],
        name="sections_" + "_".join(map(str, sections)),
    )(*operands)


def body(features, tiles, tile_cols, tile_ptr):
    size = tiles.shape[1]
    width = features.shape[1]
    rows = lax.axis_size("rows")
    reps = lax.axis_size("reps")
    sections = rows // reps
    line = rows // 4

    def aligned(row, rep):
        return row + sections * rep + MIDDLE, rep

    def step(distance):
        return lambda row, rep: (row + distance, rep)

    def step_in_line(distance):
        def source(row, rep):
            base, at = row // line * line, row % line
            if 0 <= at + distance < line:
                return row + distance, rep
            turn = line // sections if distance > 0 else -(line // sections)
            return base + (at + distance) % line, rep + turn

        return source

    middle = moved(features, rows, reps, aligned)
    far = moved(middle, rows, reps, step_in_line(2))
    after = moved(middle, rows, reps, step(1))
    before = moved(middle, rows, reps, step(-1))
    partial = sections_sum((1, 0, 2), tile_cols, tile_ptr, tiles, (middle, before, after))
    partial = sections_sum((3,), tile_cols, tile_ptr, tiles, (far,), partial)
    blocks = partial.reshape(reps, size, width)
    arrived = lax.all_to_all(blocks, "reps", split_axis=0, concat_axis=0, tiled=True)
    return arrived.sum(axis=0).astype(jnp.bfloat16)


def solution(mesh):
    placed = (
        P("rows", "cols"),
        P(("rows", "reps"), None, None),
        P(("rows", "reps"), None),
        P(("rows", "reps"), None),
    )
    return jax.shard_map(
        body, mesh=mesh, in_specs=placed, out_specs=P(("rows", "reps"), "cols"), check_vma=False
    )
```

```python
import functools

import jax
import jax.numpy as jnp
from jax import lax
from jax.experimental import pallas as pl
from jax.experimental.pallas import tpu as pltpu
from jax.sharding import PartitionSpec as P


TB = 8
CENTRE = 2
MIB = 1 << 20


def moved(block, rows, reps, source):
    route = []
    for row in range(rows):
        for rep in range(reps):
            from_row, from_rep = source(row, rep)
            route.append((from_row % rows * reps + from_rep % reps, row * reps + rep))
    return lax.ppermute(block, ("rows", "reps"), route)


def dense_kernel(sections, cols, ptr, tiles, dense, sem):
    size = tiles.shape[1]
    dense[...] = jnp.zeros(dense.shape, dense.dtype)

    def tile_copy(slot, section, row, entry):
        where = dense.at[
            section, pl.ds(row * size, size), pl.ds(pl.multiple_of(entry * size, size), size)
        ]
        return pltpu.make_async_copy(tiles.at[slot], where, sem)

    for section in range(sections):
        for row in range(TB):
            key = section * TB + row

            def send(slot, carry, section=section, row=row):
                tile_copy(slot, section, row, lax.rem(cols[0, slot], TB)).start()
                return carry

            lax.fori_loop(ptr[0, key], ptr[0, key + 1], send, 0)

    def arrive(slot, carry):
        tile_copy(0, 0, 0, 0).wait()
        return carry

    lax.fori_loop(0, ptr[0, sections * TB], arrive, 0)


def dense_sections(sections, cols, ptr, tiles):
    size = tiles.shape[1]
    scalars = pl.BlockSpec(memory_space=pltpu.SMEM)
    return pl.pallas_call(
        functools.partial(dense_kernel, sections),
        out_shape=pltpu.VMEM((sections, TB * size, TB * size), tiles.dtype),
        in_specs=[scalars, scalars, pl.BlockSpec(memory_space=pl.ANY)],
        out_specs=pl.BlockSpec(memory_space=pltpu.VMEM),
        scratch_shapes=[pltpu.SemaphoreType.DMA],
        compiler_params=pltpu.CompilerParams(vmem_limit_bytes=12 * MIB),
        name="dense_sections",
    )(cols, ptr, pltpu.with_memory_space_constraint(tiles, pltpu.HBM))


def product_kernel(sections, chained, dense, *refs):
    feats = refs[: len(sections)]
    total = refs[-1]
    value = refs[len(sections)][...] if chained else None
    for at, section in enumerate(sections):
        part = jnp.dot(dense[section], feats[at][...], preferred_element_type=jnp.float32)
        value = part if value is None else value + part
    total[...] = value


def product_sum(sections, dense, feats, start=None):
    operands = [dense, *feats] + ([] if start is None else [start])
    operands = [pltpu.with_memory_space_constraint(x, pltpu.VMEM) for x in operands]
    whole = pl.BlockSpec(memory_space=pltpu.VMEM)
    return pl.pallas_call(
        functools.partial(product_kernel, sections, start is not None),
        out_shape=pltpu.VMEM((dense.shape[1], feats[0].shape[1]), jnp.float32),
        in_specs=[whole] * len(operands),
        out_specs=whole,
        compiler_params=pltpu.CompilerParams(vmem_limit_bytes=16 * MIB),
    )(*operands)


def body(features, tiles, tile_cols, tile_ptr):
    size = tiles.shape[1]
    width = features.shape[1]
    rows = lax.axis_size("rows")
    reps = lax.axis_size("reps")
    sections = rows // reps
    line = rows // 4

    def aligned(section):
        return lambda row, rep: (row + sections * rep + section, rep)

    def step(distance):
        return lambda row, rep: (row + distance, rep)

    def step_in_line(distance):
        def source(row, rep):
            base, at = row // line * line, row % line
            if 0 <= at + distance < line:
                return row + distance, rep
            turn = line // sections if distance > 0 else -(line // sections)
            return base + (at + distance) % line, rep + turn

        return source

    dense = dense_sections(sections, tile_cols, tile_ptr, tiles)
    centre = moved(features, rows, reps, aligned(CENTRE))
    first = moved(features, rows, reps, aligned(0))
    after = moved(centre, rows, reps, step(1))
    before = moved(centre, rows, reps, step_in_line(-1))
    partial = product_sum((CENTRE, 0), dense, (centre, first))
    partial = product_sum((CENTRE + 1, CENTRE - 1), dense, (after, before), partial)
    blocks = partial.reshape(reps, size, width)
    arrived = lax.all_to_all(blocks, "reps", split_axis=0, concat_axis=0, tiled=True)
    return arrived.sum(axis=0).astype(jnp.bfloat16)


def solution(mesh):
    placed = (
        P("rows", "cols"),
        P(("rows", "reps"), None, None),
        P(("rows", "reps"), None),
        P(("rows", "reps"), None),
    )
    return jax.shard_map(
        body, mesh=mesh, in_specs=placed, out_specs=P(("rows", "reps"), "cols"), check_vma=False
    )
```

```python
import functools

import jax
import jax.numpy as jnp
from jax import lax
from jax.experimental import pallas as pl
from jax.experimental.pallas import tpu as pltpu
from jax.sharding import PartitionSpec as P


TB = 8
ACROSS = 5
MIB = 1 << 20


def moved(block, sizes, source):
    rows, cols, reps = sizes

    def device(row, col, rep):
        return (row % rows * cols + col) * reps + rep % reps

    route = []
    for row in range(rows):
        for col in range(cols):
            for rep in range(reps):
                from_row, from_rep = source(row, col, rep)
                route.append((device(from_row, col, from_rep), device(row, col, rep)))
    return lax.ppermute(block, ("rows", "cols", "reps"), route)


def dense_kernel(sections, cols, ptr, tiles, dense, sem):
    size = tiles.shape[1]
    dense[...] = jnp.zeros(dense.shape, dense.dtype)

    def tile_copy(slot, section, row, entry):
        where = dense.at[
            section, pl.ds(row * size, size), pl.ds(pl.multiple_of(entry * size, size), size)
        ]
        return pltpu.make_async_copy(tiles.at[slot], where, sem)

    for section in range(sections):
        for row in range(TB):
            key = section * TB + row

            def send(slot, carry, section=section, row=row):
                tile_copy(slot, section, row, lax.rem(cols[0, slot], TB)).start()
                return carry

            lax.fori_loop(ptr[0, key], ptr[0, key + 1], send, 0)

    def arrive(slot, carry):
        tile_copy(0, 0, 0, 0).wait()
        return carry

    lax.fori_loop(0, ptr[0, sections * TB], arrive, 0)


def dense_sections(sections, cols, ptr, tiles):
    size = tiles.shape[1]
    scalars = pl.BlockSpec(memory_space=pltpu.SMEM)
    return pl.pallas_call(
        functools.partial(dense_kernel, sections),
        out_shape=pltpu.VMEM((sections, TB * size, TB * size), tiles.dtype),
        in_specs=[scalars, scalars, pl.BlockSpec(memory_space=pl.ANY)],
        out_specs=pl.BlockSpec(memory_space=pltpu.VMEM),
        scratch_shapes=[pltpu.SemaphoreType.DMA],
        compiler_params=pltpu.CompilerParams(vmem_limit_bytes=12 * MIB),
        name="dense_sections",
    )(cols, ptr, pltpu.with_memory_space_constraint(tiles, pltpu.HBM))


def product_kernel(sections, chained, dense, *refs):
    feats = refs[: len(sections)]
    total = refs[-1]
    value = refs[len(sections)][...] if chained else None
    for at, section in enumerate(sections):
        part = jnp.dot(dense[section], feats[at][...], preferred_element_type=jnp.float32)
        value = part if value is None else value + part
    total[...] = value


def product_sum(sections, dense, feats, start=None):
    operands = [dense, *feats] + ([] if start is None else [start])
    operands = [pltpu.with_memory_space_constraint(x, pltpu.VMEM) for x in operands]
    whole = pl.BlockSpec(memory_space=pltpu.VMEM)
    return pl.pallas_call(
        functools.partial(product_kernel, sections, start is not None),
        out_shape=pltpu.VMEM((dense.shape[1], feats[0].shape[1]), jnp.float32),
        in_specs=[whole] * len(operands),
        out_specs=whole,
        compiler_params=pltpu.CompilerParams(vmem_limit_bytes=16 * MIB),
    )(*operands)


def body(features, tiles, tile_cols, tile_ptr):
    size = tiles.shape[1]
    width = features.shape[1]
    sizes = [lax.axis_size(axis) for axis in ("rows", "cols", "reps")]
    rows, _, reps = sizes
    sections = rows // reps

    def owner(section):
        def source(row, col, rep):
            across = (col + section) % 2 == 1
            return row + sections * rep + section, rep ^ ACROSS if across else rep

        return source

    dense = dense_sections(sections, tile_cols, tile_ptr, tiles)
    feats = []
    for section in range(sections):
        feats.append(moved(features, sizes, owner(section)))
    half = sections // 2
    partial = None
    for begin in (0, half):
        chosen = tuple(range(begin, begin + half))
        partial = product_sum(chosen, dense, feats[begin : begin + half], partial)
    blocks = partial.reshape(reps, size, width)
    arrived = lax.all_to_all(blocks, "reps", split_axis=0, concat_axis=0, tiled=True)
    return arrived.sum(axis=0).astype(jnp.bfloat16)


def solution(mesh):
    placed = (
        P("rows", "cols"),
        P(("rows", "reps"), None, None),
        P(("rows", "reps"), None),
        P(("rows", "reps"), None),
    )
    return jax.shard_map(
        body, mesh=mesh, in_specs=placed, out_specs=P(("rows", "reps"), "cols"), check_vma=False
    )
```

```python
import functools

import jax
import jax.numpy as jnp
from jax import lax
from jax.experimental import pallas as pl
from jax.experimental.pallas import tpu as pltpu
from jax.sharding import PartitionSpec as P


TB = 8
ACROSS = 5
CENTRE = 2
MIB = 1 << 20


def moved(block, sizes, source):
    rows, cols, reps = sizes

    def device(row, col, rep):
        return (row % rows * cols + col) * reps + rep % reps

    route = []
    for row in range(rows):
        for col in range(cols):
            for rep in range(reps):
                from_row, from_rep = source(row, col, rep)
                route.append((device(from_row, col, from_rep), device(row, col, rep)))
    return lax.ppermute(block, ("rows", "cols", "reps"), route)


def dense_kernel(sections, cols, ptr, tiles, dense, sem):
    size = tiles.shape[1]
    dense[...] = jnp.zeros(dense.shape, dense.dtype)

    def tile_copy(slot, section, row, entry):
        where = dense.at[
            section, pl.ds(row * size, size), pl.ds(pl.multiple_of(entry * size, size), size)
        ]
        return pltpu.make_async_copy(tiles.at[slot], where, sem)

    for section in range(sections):
        for row in range(TB):
            key = section * TB + row

            def send(slot, carry, section=section, row=row):
                tile_copy(slot, section, row, lax.rem(cols[0, slot], TB)).start()
                return carry

            lax.fori_loop(ptr[0, key], ptr[0, key + 1], send, 0)

    def arrive(slot, carry):
        tile_copy(0, 0, 0, 0).wait()
        return carry

    lax.fori_loop(0, ptr[0, sections * TB], arrive, 0)


def dense_sections(sections, cols, ptr, tiles):
    size = tiles.shape[1]
    scalars = pl.BlockSpec(memory_space=pltpu.SMEM)
    return pl.pallas_call(
        functools.partial(dense_kernel, sections),
        out_shape=pltpu.VMEM((sections, TB * size, TB * size), tiles.dtype),
        in_specs=[scalars, scalars, pl.BlockSpec(memory_space=pl.ANY)],
        out_specs=pl.BlockSpec(memory_space=pltpu.VMEM),
        scratch_shapes=[pltpu.SemaphoreType.DMA],
        compiler_params=pltpu.CompilerParams(vmem_limit_bytes=12 * MIB),
        name="dense_sections",
    )(cols, ptr, pltpu.with_memory_space_constraint(tiles, pltpu.HBM))


def product_kernel(sections, chained, dense, *refs):
    feats = refs[: len(sections)]
    total = refs[-1]
    value = refs[len(sections)][...] if chained else None
    for at, section in enumerate(sections):
        part = jnp.dot(dense[section], feats[at][...], preferred_element_type=jnp.float32)
        value = part if value is None else value + part
    total[...] = value


def product_sum(sections, dense, feats, start=None):
    operands = [dense, *feats] + ([] if start is None else [start])
    operands = [pltpu.with_memory_space_constraint(x, pltpu.VMEM) for x in operands]
    whole = pl.BlockSpec(memory_space=pltpu.VMEM)
    return pl.pallas_call(
        functools.partial(product_kernel, sections, start is not None),
        out_shape=pltpu.VMEM((dense.shape[1], feats[0].shape[1]), jnp.float32),
        in_specs=[whole] * len(operands),
        out_specs=whole,
        compiler_params=pltpu.CompilerParams(vmem_limit_bytes=16 * MIB),
    )(*operands)


def body(features, tiles, tile_cols, tile_ptr):
    size = tiles.shape[1]
    width = features.shape[1]
    sizes = [lax.axis_size(axis) for axis in ("rows", "cols", "reps")]
    rows, _, reps = sizes
    sections = rows // reps

    line = rows // 4

    def owner(section, crossing):
        def source(row, col, rep):
            across = col % 2 == crossing
            return row + sections * rep + section, rep ^ ACROSS if across else rep

        return source

    def neighbour(distance, turning):
        turn = distance * line // sections

        def source(row, col, rep):
            at = row % line + distance
            if col % 2 == turning and not 0 <= at < line:
                return row - row % line + at % line, rep + turn
            return row + distance, rep

        return source

    dense = dense_sections(sections, tile_cols, tile_ptr, tiles)
    centre = moved(features, sizes, owner(CENTRE, 1))
    first = moved(features, sizes, owner(0, 0))
    after = moved(centre, sizes, neighbour(1, 0))
    before = moved(centre, sizes, neighbour(-1, 1))
    partial = product_sum((CENTRE, 0), dense, (centre, first))
    partial = product_sum((CENTRE + 1, CENTRE - 1), dense, (after, before), partial)
    blocks = partial.reshape(reps, size, width)
    arrived = lax.all_to_all(blocks, "reps", split_axis=0, concat_axis=0, tiled=True)
    return arrived.sum(axis=0).astype(jnp.bfloat16)


def solution(mesh):
    placed = (
        P("rows", "cols"),
        P(("rows", "reps"), None, None),
        P(("rows", "reps"), None),
        P(("rows", "reps"), None),
    )
    return jax.shard_map(
        body, mesh=mesh, in_specs=placed, out_specs=P(("rows", "reps"), "cols"), check_vma=False
    )
```

```python
import functools

import jax
import jax.numpy as jnp
from jax import lax
from jax.experimental import pallas as pl
from jax.experimental.pallas import tpu as pltpu
from jax.sharding import PartitionSpec as P


TB = 8
ACROSS = 1
CENTRE = 2
MIB = 1 << 20


def moved(block, sizes, source):
    rows, cols, reps = sizes

    def device(row, col, rep):
        return (row % rows * cols + col) * reps + rep % reps

    route = []
    for row in range(rows):
        for col in range(cols):
            for rep in range(reps):
                from_row, from_rep = source(row, col, rep)
                route.append((device(from_row, col, from_rep), device(row, col, rep)))
    return lax.ppermute(block, ("rows", "cols", "reps"), route)


def dense_kernel(sections, cols, ptr, tiles, dense, col_ids, pointers, table_sems, sem):
    size = tiles.shape[1]
    tables = [
        pltpu.make_async_copy(cols, col_ids, table_sems.at[0]),
        pltpu.make_async_copy(ptr, pointers, table_sems.at[1]),
    ]
    for table in tables:
        table.start()
    dense[...] = jnp.zeros(dense.shape, dense.dtype)
    for table in tables:
        table.wait()

    def tile_copy(slot, at, row, entry):
        where = dense.at[
            at, pl.ds(row * size, size), pl.ds(pl.multiple_of(entry * size, size), size)
        ]
        return pltpu.make_async_copy(tiles.at[slot], where, sem)

    for at, section in enumerate(sections):
        for row in range(TB):
            key = section * TB + row

            def send(slot, carry, at=at, row=row):
                tile_copy(slot, at, row, lax.rem(col_ids[0, slot], TB)).start()
                return carry

            lax.fori_loop(pointers[0, key], pointers[0, key + 1], send, 0)

    def arrive(slot, carry):
        tile_copy(0, 0, 0, 0).wait()
        return carry

    for section in sections:
        lax.fori_loop(pointers[0, section * TB], pointers[0, section * TB + TB], arrive, 0)


def dense_sections(sections, cols, ptr, tiles):
    size = tiles.shape[1]
    operands = [pltpu.with_memory_space_constraint(x, pltpu.HBM) for x in (cols, ptr, tiles)]
    return pl.pallas_call(
        functools.partial(dense_kernel, sections),
        out_shape=pltpu.VMEM((len(sections), TB * size, TB * size), tiles.dtype),
        in_specs=[pl.BlockSpec(memory_space=pl.ANY)] * 3,
        out_specs=pl.BlockSpec(memory_space=pltpu.VMEM),
        scratch_shapes=[
            pltpu.SMEM(cols.shape, cols.dtype),
            pltpu.SMEM(ptr.shape, ptr.dtype),
            pltpu.SemaphoreType.DMA((2,)),
            pltpu.SemaphoreType.DMA,
        ],
        compiler_params=pltpu.CompilerParams(vmem_limit_bytes=12 * MIB),
    )(*operands)


def product_kernel(count, chained, dense, *refs):
    feats = refs[:count]
    total = refs[-1]
    value = refs[count][...] if chained else None
    for at in range(count):
        part = jnp.dot(dense[at], feats[at][...], preferred_element_type=jnp.float32)
        value = part if value is None else value + part
    total[...] = value


def product_sum(dense, feats, start=None):
    operands = [dense, *feats] + ([] if start is None else [start])
    operands = [pltpu.with_memory_space_constraint(x, pltpu.VMEM) for x in operands]
    whole = pl.BlockSpec(memory_space=pltpu.VMEM)
    return pl.pallas_call(
        functools.partial(product_kernel, len(feats), start is not None),
        out_shape=pltpu.VMEM((dense.shape[1], feats[0].shape[1]), jnp.float32),
        in_specs=[whole] * len(operands),
        out_specs=whole,
        compiler_params=pltpu.CompilerParams(vmem_limit_bytes=16 * MIB),
    )(*operands)


def body(features, tiles, tile_cols, tile_ptr):
    size = tiles.shape[1]
    width = features.shape[1]
    sizes = [lax.axis_size(axis) for axis in ("rows", "cols", "reps")]
    rows, _, reps = sizes
    sections = rows // reps

    line = rows // 4

    def owner(section, crossing):
        def source(row, col, rep):
            across = col % 2 == crossing
            return row + sections * rep + section, rep ^ ACROSS if across else rep

        return source

    def neighbour(distance, turning):
        turn = distance * line // sections

        def source(row, col, rep):
            at = row % line + distance
            if col % 2 == turning and not 0 <= at < line:
                return row - row % line + at % line, rep + turn
            return row + distance, rep

        return source

    early, late = (CENTRE, 0), (CENTRE + 1, CENTRE - 1)
    dense_early = dense_sections(early, tile_cols, tile_ptr, tiles)
    dense_late = dense_sections(late, tile_cols, tile_ptr, tiles)
    centre = moved(features, sizes, owner(CENTRE, 1))
    first = moved(features, sizes, owner(0, 0))
    after = moved(centre, sizes, neighbour(1, 0))
    before = moved(centre, sizes, neighbour(-1, 1))
    partial = product_sum(dense_early, (centre, first))
    partial = product_sum(dense_late, (after, before), partial)
    blocks = partial.reshape(reps, size, width)
    arrived = lax.all_to_all(blocks, "reps", split_axis=0, concat_axis=0, tiled=True)
    return arrived.sum(axis=0).astype(jnp.bfloat16)


def solution(mesh):
    placed = (
        P("rows", "cols"),
        P(("rows", "reps"), None, None),
        P(("rows", "reps"), None),
        P(("rows", "reps"), None),
    )
    return jax.shard_map(
        body, mesh=mesh, in_specs=placed, out_specs=P(("rows", "reps"), "cols"), check_vma=False
    )
```

```python
import functools

import jax
import jax.numpy as jnp
from jax import lax
from jax.experimental import pallas as pl
from jax.experimental.pallas import tpu as pltpu
from jax.sharding import PartitionSpec as P


TB = 8
NEAR_PLANE = 1
FAR_PLANE = 5
CENTRE = 2
MIB = 1 << 20


def moved(block, sizes, source):
    rows, cols, reps = sizes

    def device(row, col, rep):
        return (row % rows * cols + col) * reps + rep % reps

    route = []
    for row in range(rows):
        for col in range(cols):
            for rep in range(reps):
                from_row, from_rep = source(row, col, rep)
                route.append((device(from_row, col, from_rep), device(row, col, rep)))
    return lax.ppermute(block, ("rows", "cols", "reps"), route)


def dense_kernel(sections, cols, ptr, tiles, dense, col_ids, pointers, table_sems, sem):
    size = tiles.shape[1]
    tables = [
        pltpu.make_async_copy(cols, col_ids, table_sems.at[0]),
        pltpu.make_async_copy(ptr, pointers, table_sems.at[1]),
    ]
    for table in tables:
        table.start()
    dense[...] = jnp.zeros(dense.shape, dense.dtype)
    for table in tables:
        table.wait()

    def tile_copy(slot, at, row, entry):
        where = dense.at[
            at, pl.ds(row * size, size), pl.ds(pl.multiple_of(entry * size, size), size)
        ]
        return pltpu.make_async_copy(tiles.at[slot], where, sem)

    for at, section in enumerate(sections):
        for row in range(TB):
            key = section * TB + row

            def send(slot, carry, at=at, row=row):
                tile_copy(slot, at, row, lax.rem(col_ids[0, slot], TB)).start()
                return carry

            lax.fori_loop(pointers[0, key], pointers[0, key + 1], send, 0)

    def arrive(slot, carry):
        tile_copy(0, 0, 0, 0).wait()
        return carry

    for section in sections:
        lax.fori_loop(pointers[0, section * TB], pointers[0, section * TB + TB], arrive, 0)


def dense_sections(sections, cols, ptr, tiles):
    size = tiles.shape[1]
    operands = [pltpu.with_memory_space_constraint(x, pltpu.HBM) for x in (cols, ptr, tiles)]
    return pl.pallas_call(
        functools.partial(dense_kernel, sections),
        out_shape=pltpu.VMEM((len(sections), TB * size, TB * size), tiles.dtype),
        in_specs=[pl.BlockSpec(memory_space=pl.ANY)] * 3,
        out_specs=pl.BlockSpec(memory_space=pltpu.VMEM),
        scratch_shapes=[
            pltpu.SMEM(cols.shape, cols.dtype),
            pltpu.SMEM(ptr.shape, ptr.dtype),
            pltpu.SemaphoreType.DMA((2,)),
            pltpu.SemaphoreType.DMA,
        ],
        compiler_params=pltpu.CompilerParams(vmem_limit_bytes=12 * MIB),
    )(*operands)


def product_kernel(count, chained, dense, *refs):
    feats = refs[:count]
    total = refs[-1]
    value = refs[count][...] if chained else None
    for at in range(count):
        part = jnp.dot(dense[at], feats[at][...], preferred_element_type=jnp.float32)
        value = part if value is None else value + part
    total[...] = value


def product_sum(dense, feats, start=None):
    operands = [dense, *feats] + ([] if start is None else [start])
    operands = [pltpu.with_memory_space_constraint(x, pltpu.VMEM) for x in operands]
    whole = pl.BlockSpec(memory_space=pltpu.VMEM)
    return pl.pallas_call(
        functools.partial(product_kernel, len(feats), start is not None),
        out_shape=pltpu.VMEM((dense.shape[1], feats[0].shape[1]), jnp.float32),
        in_specs=[whole] * len(operands),
        out_specs=whole,
        compiler_params=pltpu.CompilerParams(vmem_limit_bytes=16 * MIB),
    )(*operands)


def body(features, tiles, tile_cols, tile_ptr):
    size = tiles.shape[1]
    width = features.shape[1]
    sizes = [lax.axis_size(axis) for axis in ("rows", "cols", "reps")]
    rows, _, reps = sizes
    sections = rows // reps

    line = rows // 4

    def owner(section, crossing, plane):
        def source(row, col, rep):
            across = col % 2 == crossing
            return row + sections * rep + section, rep ^ plane if across else rep

        return source

    def neighbour(distance, turning):
        turn = distance * line // sections

        def source(row, col, rep):
            at = row % line + distance
            if col % 2 == turning and not 0 <= at < line:
                return row - row % line + at % line, rep + turn
            return row + distance, rep

        return source

    early, late = (CENTRE, 0), (CENTRE + 1, CENTRE - 1)
    dense_early = dense_sections(early, tile_cols, tile_ptr, tiles)
    dense_late = dense_sections(late, tile_cols, tile_ptr, tiles)
    centre = moved(features, sizes, owner(CENTRE, 1, NEAR_PLANE))
    first = moved(features, sizes, owner(0, 0, FAR_PLANE))
    after = moved(centre, sizes, neighbour(1, 0))
    before = moved(centre, sizes, neighbour(-1, 1))
    partial = product_sum(dense_early, (centre, first))
    partial = product_sum(dense_late, (after, before), partial)
    blocks = partial.reshape(reps, size, width)
    arrived = lax.all_to_all(blocks, "reps", split_axis=0, concat_axis=0, tiled=True)
    return arrived.sum(axis=0).astype(jnp.bfloat16)


def solution(mesh):
    placed = (
        P("rows", "cols"),
        P(("rows", "reps"), None, None),
        P(("rows", "reps"), None),
        P(("rows", "reps"), None),
    )
    return jax.shard_map(
        body, mesh=mesh, in_specs=placed, out_specs=P(("rows", "reps"), "cols"), check_vma=False
    )
```

```python
import functools

import jax
import jax.numpy as jnp
from jax import lax
from jax.experimental import pallas as pl
from jax.experimental.pallas import tpu as pltpu
from jax.sharding import PartitionSpec as P


TB = 8
NEAR_PLANE = 1
FAR_PLANE = 5
CENTRE = 2
MIB = 1 << 20


def moved(block, sizes, source):
    rows, cols, reps = sizes

    def device(row, col, rep):
        return (row % rows * cols + col) * reps + rep % reps

    route = []
    for row in range(rows):
        for col in range(cols):
            for rep in range(reps):
                from_row, from_rep = source(row, col, rep)
                route.append((device(from_row, col, from_rep), device(row, col, rep)))
    return lax.ppermute(block, ("rows", "cols", "reps"), route)


def dense_kernel(sections, cols, ptr, tiles, dense, col_ids, pointers, table_sems, sem):
    size = tiles.shape[1]
    tables = [
        pltpu.make_async_copy(cols, col_ids, table_sems.at[0]),
        pltpu.make_async_copy(ptr, pointers, table_sems.at[1]),
    ]
    for table in tables:
        table.start()
    dense[...] = jnp.zeros(dense.shape, dense.dtype)
    for table in tables:
        table.wait()

    def tile_copy(slot, at, row, entry):
        where = dense.at[
            at, pl.ds(row * size, size), pl.ds(pl.multiple_of(entry * size, size), size)
        ]
        return pltpu.make_async_copy(tiles.at[slot], where, sem)

    for at, section in enumerate(sections):
        for row in range(TB):
            key = section * TB + row

            def send(slot, carry, at=at, row=row):
                tile_copy(slot, at, row, lax.rem(col_ids[0, slot], TB)).start()
                return carry

            lax.fori_loop(pointers[0, key], pointers[0, key + 1], send, 0)

    def arrive(slot, carry):
        tile_copy(0, 0, 0, 0).wait()
        return carry

    for section in sections:
        lax.fori_loop(pointers[0, section * TB], pointers[0, section * TB + TB], arrive, 0)


def dense_sections(sections, cols, ptr, tiles):
    size = tiles.shape[1]
    operands = [pltpu.with_memory_space_constraint(x, pltpu.HBM) for x in (cols, ptr, tiles)]
    return pl.pallas_call(
        functools.partial(dense_kernel, sections),
        out_shape=pltpu.VMEM((len(sections), TB * size, TB * size), tiles.dtype),
        in_specs=[pl.BlockSpec(memory_space=pl.ANY)] * 3,
        out_specs=pl.BlockSpec(memory_space=pltpu.VMEM),
        scratch_shapes=[
            pltpu.SMEM(cols.shape, cols.dtype),
            pltpu.SMEM(ptr.shape, ptr.dtype),
            pltpu.SemaphoreType.DMA((2,)),
            pltpu.SemaphoreType.DMA,
        ],
        compiler_params=pltpu.CompilerParams(vmem_limit_bytes=12 * MIB),
    )(*operands)


def product_kernel(offset, count, chained, dense, *refs):
    feats = refs[:count]
    total = refs[-1]
    value = refs[count][...] if chained else None
    for at in range(count):
        part = jnp.dot(dense[offset + at], feats[at][...], preferred_element_type=jnp.float32)
        value = part if value is None else value + part
    total[...] = value


def product_sum(dense, feats, start=None, offset=0):
    operands = [dense, *feats] + ([] if start is None else [start])
    operands = [pltpu.with_memory_space_constraint(x, pltpu.VMEM) for x in operands]
    whole = pl.BlockSpec(memory_space=pltpu.VMEM)
    return pl.pallas_call(
        functools.partial(product_kernel, offset, len(feats), start is not None),
        out_shape=pltpu.VMEM((dense.shape[1], feats[0].shape[1]), jnp.float32),
        in_specs=[whole] * len(operands),
        out_specs=whole,
        compiler_params=pltpu.CompilerParams(vmem_limit_bytes=16 * MIB),
    )(*operands)


def body(features, tiles, tile_cols, tile_ptr):
    size = tiles.shape[1]
    width = features.shape[1]
    sizes = [lax.axis_size(axis) for axis in ("rows", "cols", "reps")]
    rows, _, reps = sizes
    sections = rows // reps

    line = rows // 4

    def owner(section, crossing, plane):
        def source(row, col, rep):
            across = col % 2 == crossing
            return row + sections * rep + section, rep ^ plane if across else rep

        return source

    def neighbour(distance, turning):
        turn = distance * line // sections

        def source(row, col, rep):
            at = row % line + distance
            if col % 2 == turning and not 0 <= at < line:
                return row - row % line + at % line, rep + turn
            return row + distance, rep

        return source

    early, late = (CENTRE, 0), (CENTRE + 1, CENTRE - 1)
    dense_early = dense_sections(early, tile_cols, tile_ptr, tiles)
    dense_late = dense_sections(late, tile_cols, tile_ptr, tiles)
    centre = moved(features, sizes, owner(CENTRE, 1, NEAR_PLANE))
    first = moved(features, sizes, owner(0, 0, FAR_PLANE))
    after = moved(centre, sizes, neighbour(1, 0))
    before = moved(centre, sizes, neighbour(-1, 1))
    partial = product_sum(dense_early, (centre, first))
    partial = product_sum(dense_late, (before,), partial, 1)
    partial = product_sum(dense_late, (after,), partial)
    blocks = partial.reshape(reps, size, width)
    arrived = lax.all_to_all(blocks, "reps", split_axis=0, concat_axis=0, tiled=True)
    return arrived.sum(axis=0).astype(jnp.bfloat16)


def solution(mesh):
    placed = (
        P("rows", "cols"),
        P(("rows", "reps"), None, None),
        P(("rows", "reps"), None),
        P(("rows", "reps"), None),
    )
    return jax.shard_map(
        body, mesh=mesh, in_specs=placed, out_specs=P(("rows", "reps"), "cols"), check_vma=False
    )
```
